8 devices in a mesh: dp: 2 (over z, y), tp: 4 (over x, core).
Axes of the slice: x: 2, y: 2, z: 1, core: 2. Of those that a mesh axis runs over, the one named last changes fastest.
Arguments:
- residual: bfloat16 [512, 4096], P('dp'), parts along dimension 0
- positions: int32 [512], P('dp'), parts along dimension 0
- k_cache: bfloat16 [2, 512, 8, 64, 128], P(None, 'dp', 'tp'), parts along dimension 1
- v_cache: bfloat16 [2, 512, 8, 64, 128], P(None, 'dp', 'tp'), parts along dimension 1
- ln_weight: bfloat16 [2, 4096], replicated
- w_q: bfloat16 [2, 4096, 4096], P(None, None, 'tp')
- w_k: bfloat16 [2, 4096, 1024], P(None, None, 'tp')
- w_v: bfloat16 [2, 4096, 1024], P(None, None, 'tp')
- q_norm_w: bfloat16 [2, 32, 128], P(None, 'tp')
- k_norm_w: bfloat16 [2, 8, 128], P(None, 'tp')
- w_o: bfloat16 [2, 4096, 4096], P(None, 'tp')
- w_gate: bfloat16 [2, 4096, 14336], P(None, None, 'tp')
- w_up: bfloat16 [2, 4096, 14336], P(None, None, 'tp')
- w_down: bfloat16 [2, 14336, 4096], P(None, 'tp')
Outputs:
- output 1: bfloat16 [512, 4096], P('dp'), parts along dimension 0
- output 2: bfloat16 [2, 512, 8, 64, 128], P(None, 'dp', 'tp'), parts along dimension 1
- output 3: bfloat16 [2, 512, 8, 64, 128], P(None, 'dp', 'tp'), parts along dimension 1
There are 2 independent parts. The reference program is written for one: setup_inputs(seed, part) draws one part's arguments, and reference() takes and returns one part's arrays. A program takes and returns all parts, laid end to end along the dimension named above; an argument that names none is the same for every part.
All inputs are finite; a program needn't handle non-finite values.
Results may differ from the reference program's by a relative error of at most 0.016126.
Values are sent between devices in bfloat16 or wider.
A program may use at most 1.25 GiB of HBM per device.

```python
import math
import jax
import jax.numpy as jnp
from jax import lax

D = 4096
HEADS = 32
KV_HEADS = 8
HEAD = 128
FF = 14336
BATCH = 256
SEQ = 64
LAYERS = 2
EPS = 1e-5
ROPE_THETA = 75000000.0
GROUP = HEADS // KV_HEADS


def cohere_norm(values, weight):
    centered = values - jnp.mean(values, axis=-1, keepdims=True)
    variance = jnp.mean(centered * centered, axis=-1, keepdims=True)
    return centered * lax.rsqrt(variance + EPS) * weight.astype(jnp.float32)


def rotate(values, cos_t, sin_t):
    paired = values.reshape(values.shape[:-1] + (values.shape[-1] // 2, 2))
    even_part = paired[..., 0]
    odd_part = paired[..., 1]
    turned = jnp.stack([even_part * cos_t - odd_part * sin_t, odd_part * cos_t + even_part * sin_t], axis=-1)
    return turned.reshape(values.shape)


def draw_normal(rng_key, arr_shape, scale_factor):
    return (scale_factor * jax.random.normal(rng_key, arr_shape, jnp.float32)).astype(jnp.bfloat16)


def setup_inputs(seed: int = 0, part: int = 0) -> dict:
    base_key = jax.random.key(seed)
    shared_keys = jax.random.split(base_key, 10)
    local_keys = jax.random.split(jax.random.fold_in(base_key, part), 4)
    key_scale = math.sqrt(0.8 * math.log(SEQ))
    q_cols = HEADS * HEAD
    kv_cols = KV_HEADS * HEAD
    cache_shape = (LAYERS, BATCH, KV_HEADS, SEQ, HEAD)
    positions = jax.random.randint(local_keys[0], (BATCH,), SEQ // 2, SEQ, dtype=jnp.int32)
    positions = positions.at[0].set(SEQ - 1).at[1].set(SEQ // 2)
    return {
        "residual": draw_normal(local_keys[1], (BATCH, D), 1.0),
        "positions": positions,
        "k_cache": draw_normal(local_keys[2], cache_shape, key_scale),
        "v_cache": draw_normal(local_keys[3], cache_shape, 1.0),
        "ln_weight": (1.0 + 0.2 * jax.random.normal(shared_keys[0], (LAYERS, D), jnp.float32)).astype(jnp.bfloat16),
        "w_q": draw_normal(shared_keys[1], (LAYERS, D, q_cols), D ** -0.5),
        "w_k": draw_normal(shared_keys[2], (LAYERS, D, kv_cols), D ** -0.5),
        "w_v": draw_normal(shared_keys[3], (LAYERS, D, kv_cols), D ** -0.5),
        "q_norm_w": (1.0 + 0.3 * jax.random.normal(shared_keys[4], (LAYERS, HEADS, HEAD), jnp.float32)).astype(jnp.bfloat16),
        "k_norm_w": (key_scale * (1.0 + 0.3 * jax.random.normal(shared_keys[5], (LAYERS, KV_HEADS, HEAD), jnp.float32))).astype(jnp.bfloat16),
        "w_o": draw_normal(shared_keys[6], (LAYERS, q_cols, D), q_cols ** -0.5),
        "w_gate": draw_normal(shared_keys[7], (LAYERS, D, FF), D ** -0.5),
        "w_up": draw_normal(shared_keys[8], (LAYERS, D, FF), D ** -0.5),
        "w_down": draw_normal(shared_keys[9], (LAYERS, FF, D), FF ** -0.5),
    }


def reference(residual, positions, k_cache, v_cache, ln_weight, w_q, w_k, w_v, q_norm_w, k_norm_w, w_o, w_gate, w_up, w_down):
    half_ids = jnp.arange(HEAD // 2, dtype=jnp.float32)
    inv_freq = ROPE_THETA ** (-2.0 * half_ids / HEAD)
    angles = positions.astype(jnp.float32)[:, None] * inv_freq[None, :]
    cos_t = jnp.cos(angles)[:, None, :]
    sin_t = jnp.sin(angles)[:, None, :]
    seq_ids = jnp.arange(SEQ)
    at_pos = seq_ids[None, None, :, None] == positions[:, None, None, None]
    visible = seq_ids[None, None, None, :] <= positions[:, None, None, None]
    score_scale = 1.0 / math.sqrt(HEAD)

    def layer_body(resid_x, layer_params):
        (layer_ln, layer_wq, layer_wk, layer_wv, layer_qn, layer_kn, layer_wo, layer_wg, layer_wu, layer_wd, layer_kc, layer_vc) = layer_params
        hidden = cohere_norm(resid_x.astype(jnp.float32), layer_ln).astype(jnp.bfloat16)
        q_proj = jnp.dot(hidden, layer_wq, preferred_element_type=jnp.float32).astype(jnp.bfloat16)
        k_proj = jnp.dot(hidden, layer_wk, preferred_element_type=jnp.float32).astype(jnp.bfloat16)
        v_proj = jnp.dot(hidden, layer_wv, preferred_element_type=jnp.float32).astype(jnp.bfloat16).reshape(BATCH, KV_HEADS, HEAD)
        q_rot = rotate(cohere_norm(q_proj.reshape(BATCH, HEADS, HEAD).astype(jnp.float32), layer_qn), cos_t, sin_t).astype(jnp.bfloat16)
        k_rot = rotate(cohere_norm(k_proj.reshape(BATCH, KV_HEADS, HEAD).astype(jnp.float32), layer_kn), cos_t, sin_t).astype(jnp.bfloat16)
        k_upd = jnp.where(at_pos, k_rot[:, :, None, :], layer_kc)
        v_upd = jnp.where(at_pos, v_proj[:, :, None, :], layer_vc)
        q_grouped = q_rot.reshape(BATCH, KV_HEADS, GROUP, HEAD).astype(jnp.float32)
        scores = jnp.einsum("bkgd,bksd->bkgs", q_grouped, k_upd.astype(jnp.float32)) * score_scale
        scores = jnp.where(visible, scores, -1e30)
        attn_probs = jax.nn.softmax(scores, axis=-1).astype(jnp.bfloat16)
        attn_heads = jnp.einsum("bkgs,bksd->bkgd", attn_probs.astype(jnp.float32), v_upd.astype(jnp.float32)).astype(jnp.bfloat16).reshape(BATCH, HEADS * HEAD)
        attn_out = jnp.dot(attn_heads, layer_wo, preferred_element_type=jnp.float32)
        gate_proj = jnp.dot(hidden, layer_wg, preferred_element_type=jnp.float32).astype(jnp.bfloat16)
        up_proj = jnp.dot(hidden, layer_wu, preferred_element_type=jnp.float32).astype(jnp.bfloat16)
        activated = (jax.nn.silu(gate_proj.astype(jnp.float32)) * up_proj.astype(jnp.float32)).astype(jnp.bfloat16)
        mlp_out = jnp.dot(activated, layer_wd, preferred_element_type=jnp.float32)
        next_x = (resid_x.astype(jnp.float32) + attn_out + mlp_out).astype(jnp.bfloat16)
        return next_x, (k_upd, v_upd)

    final_x, (k_new, v_new) = lax.scan(layer_body, residual, (ln_weight, w_q, w_k, w_v, q_norm_w, k_norm_w, w_o, w_gate, w_up, w_down, k_cache, v_cache))
    return final_x, k_new, v_new
```

```python
import functools
import math
import jax
import jax.numpy as jnp
from jax import lax
from jax.experimental import pallas as pl
from jax.experimental.pallas import tpu as pltpu
from jax.sharding import PartitionSpec as P

EPS = 1e-5
ROPE_THETA = 75000000.0
F32 = jnp.float32
BF16 = jnp.bfloat16

ROWS = 256
D = 4096
HD = 128
QH = 8
KVH = 2
SEQ = 64
FFL = 3584
QC = QH * HD
ACTC = QC + FFL
TN = 512
NS = 8
GU = 256
N_GU = FFL // GU
CB = 16
N_CB = ROWS // CB
NC = 4
N_OUT = D // TN
HALF = ROWS // 2


def layer_norm(v, w):
    c = v - jnp.mean(v, axis=-1, keepdims=True)
    var = jnp.mean(c * c, axis=-1, keepdims=True)
    return c * lax.rsqrt(var + EPS) * w


def rope(v, cos_b, sin_b):
    even = lax.rem(lax.broadcasted_iota(jnp.int32, v.shape, 1), 2) == 0
    swapped = jnp.where(even, pltpu.roll(v, HD - 1, 1), pltpu.roll(v, 1, 1))
    return v * cos_b + swapped * sin_b


def local_kernel(l, pos_ref, ln_ref, qn_ref, kn_ref, cos_ref, sin_ref, posb_ref, x_hbm, kc, vc, wq, wk, wv, wg, wu, *rest):
    rest = rest[2:] if l else rest
    (act_hbm, k_out, v_out, x_s, h_s, q_s, k_s, v_s, act_s, w_s, kb, vb, x_sem, w_sem, ci_sem, co_sem, act_sem) = rest

    def w_pair(i, slot, a, b, off):
        return (
            pltpu.make_async_copy(a.at[l, :, pl.ds(off, GU)], w_s.at[slot, :, pl.ds(0, GU)], w_sem.at[slot, 0]),
            pltpu.make_async_copy(b.at[l, :, pl.ds(off, GU)], w_s.at[slot, :, pl.ds(GU, GU)], w_sem.at[slot, 1]),
        )

    def tile(i):
        if isinstance(i, int) and i < 2:
            return w_pair(i, i, wq.at[:, :, pl.ds(i * TN, GU)], wq.at[:, :, pl.ds(i * TN + GU, GU)], 0)
        if isinstance(i, int) and i == 2:
            return w_pair(i, i, wk, wv, 0)
        off = (i - 3) * GU
        if not isinstance(i, int):
            off = pl.multiple_of(off, GU)
        return w_pair(i, i % NS if isinstance(i, int) else lax.rem(i, NS), wg, wu, off)

    def start(i):
        for c in tile(i):
            c.start()

    def wait(i):
        for c in tile(i):
            c.wait()

    def cache_in(b, s):
        r = pl.ds(b * CB, CB)
        return (
            pltpu.make_async_copy(kc.at[l, r], kb.at[s], ci_sem.at[s, 0]),
            pltpu.make_async_copy(vc.at[l, r], vb.at[s], ci_sem.at[s, 1]),
        )

    def cache_out(b, s):
        r = pl.ds(b * CB, CB)
        return (
            pltpu.make_async_copy(kb.at[s], k_out.at[l, r], co_sem.at[s, 0]),
            pltpu.make_async_copy(vb.at[s], v_out.at[l, r], co_sem.at[s, 1]),
        )

    x_copy = pltpu.make_async_copy(x_hbm, x_s, x_sem)
    x_copy.start()
    for i in range(3):
        start(i)
    for b in range(NC - 1):
        for c in cache_in(b, b):
            c.start()
    for i in range(3, NS):
        start(i)
    x_copy.wait()

    ln_w = ln_ref[pl.ds(l, 1), :].astype(F32)

    @pl.loop(0, ROWS // 16)
    def _(r):
        rows = pl.ds(pl.multiple_of(r * 16, 16), 16)
        h_s[rows, :] = layer_norm(x_s[rows, :].astype(F32), ln_w).astype(BF16)

    @pl.loop(0, 2)
    def _(t):
        for i in range(2):
            @pl.when(t == i)
            def _():
                wait(i)
        y = jnp.dot(h_s[...], w_s[t], preferred_element_type=F32)
        start(t + NS)
        for j in range(4):
            q_s[t * 4 + j] = y[:, j * HD:(j + 1) * HD]

    wait(2)
    y = jnp.dot(h_s[...], w_s[2], preferred_element_type=F32)
    start(2 + NS)
    for j in range(2):
        k_s[j] = y[:, j * HD:(j + 1) * HD]
        v_s[j] = y[:, GU + j * HD:GU + (j + 1) * HD]

    @pl.loop(0, ROWS // 32)
    def _(r):
        rows = pl.ds(pl.multiple_of(r * 32, 32), 32)
        cb = cos_ref[rows, :]
        sb = sin_ref[rows, :]
        for src, nw, n in ((q_s, qn_ref, QH), (k_s, kn_ref, KVH)):
            for j in range(n):
                v = src[j, rows, :].astype(BF16).astype(F32)
                src[j, rows, :] = rope(layer_norm(v, nw[l, pl.ds(j, 1), :].astype(F32)), cb, sb)

    scale = 1.0 / math.sqrt(HD)
    lane = lax.broadcasted_iota(jnp.int32, (8, 8 * SEQ), 1)
    low = lax.broadcasted_iota(jnp.int32, (8, 8 * SEQ), 0) * SEQ
    sub16 = lax.broadcasted_iota(jnp.int32, (16, HD), 0)

    @pl.loop(0, N_CB)
    def _(b):
        s = lax.rem(b, NC)
        for c in cache_in(b, s):
            c.wait()
        base = pl.multiple_of(b * CB, CB)
        news = [[src[j, pl.ds(base, CB), :] for j in range(KVH)] for src in (k_s, v_s)]
        for r in range(CB):
            p = pos_ref[base + r]
            st = pl.multiple_of((p >> 4) << 4, 16)
            hit = sub16 == p - st
            for buf, new in ((kb, news[0]), (vb, news[1])):
                for j in range(KVH):
                    old = buf[s, r, j, pl.ds(st, 16), :].astype(F32)
                    fresh = jnp.broadcast_to(new[j][r:r + 1, :], (16, HD))
                    buf[s, r, j, pl.ds(st, 16), :] = jnp.where(hit, fresh, old).astype(BF16)
        for j in range(KVH):
            outs = []
            for hf in range(2):
                rows = pl.ds(pl.multiple_of(base + hf * 8, 8), 8)
                q = jnp.concatenate([q_s[j * 4 + g, rows, :] for g in range(4)], axis=0).astype(BF16)
                k = kb[s, hf * 8:(hf + 1) * 8, j].reshape(8 * SEQ, HD)
                sc = lax.dot_general(q, k, (((1,), (1,)), ((), ())), preferred_element_type=F32)
                pb = jnp.concatenate([posb_ref[rows, :]] * 4, axis=1)
                ok = (lane >= low) & (lane <= low + pb)
                probs = []
                for g in range(4):
                    z = jnp.where(ok, sc[g * 8:(g + 1) * 8, :] * scale, -1e30)
                    e = jnp.exp(z - jnp.max(z, axis=-1, keepdims=True))
                    probs.append(e / jnp.sum(e, axis=-1, keepdims=True))
                pr = jnp.concatenate(probs, axis=0).astype(BF16)
                v = vb[s, hf * 8:(hf + 1) * 8, j].reshape(8 * SEQ, HD)
                outs.append(jnp.dot(pr, v, preferred_element_type=F32))
            for g in range(4):
                o = jnp.concatenate([outs[0][g * 8:(g + 1) * 8], outs[1][g * 8:(g + 1) * 8]], axis=0)
                act_s[pl.ds(base, CB), (j * 4 + g) * HD:(j * 4 + g + 1) * HD] = o.astype(BF16)
        for c in cache_out(b, s):
            c.start()

        @pl.when(b + NC - 1 < N_CB)
        def _():
            n = lax.rem(b + NC - 1, NC)

            @pl.when(b >= 1)
            def _():
                for c in cache_out(b - 1, n):
                    c.wait()
            for c in cache_in(b + NC - 1, n):
                c.start()

    def act_copy(t):
        if isinstance(t, int) and t < 0:
            return pltpu.make_async_copy(act_s.at[:, pl.ds(0, QC)], act_hbm.at[:, pl.ds(0, QC)], act_sem.at[N_GU])
        cols = pl.ds(pl.multiple_of(QC + t * GU, GU), GU)
        return pltpu.make_async_copy(act_s.at[:, cols], act_hbm.at[:, cols], act_sem.at[t])

    act_copy(-1).start()

    @pl.loop(0, N_GU)
    def _(t):
        i = t + 3
        wait(i)
        y = jnp.dot(h_s[...], w_s[lax.rem(i, NS)], preferred_element_type=F32)

        @pl.when(i + NS < N_GU + 3)
        def _():
            start(i + NS)
        g = y[:, :GU].astype(BF16).astype(F32)
        u = y[:, GU:].astype(BF16).astype(F32)
        act_s[:, pl.ds(pl.multiple_of(QC + t * GU, GU), GU)] = (g / (1.0 + jnp.exp(-g)) * u).astype(BF16)
        act_copy(t).start()

    act_copy(-1).wait()

    @pl.loop(0, N_GU)
    def _(t):
        act_copy(t).wait()

    for b in range(N_CB - NC, N_CB):
        for c in cache_out(b, b % NC):
            c.wait()


def reduce_kernel(l, act_hbm, x_hbm, wo, wd, out_hbm, act_s, x_s, w_s, part, recv1, send2, recv2, xnew, a_sem, w_sem, s1, r1, s2, r2, s3, r3, o_sem):
    me = lax.axis_index("tp")
    core = lax.rem(me, 2)
    sib = me + 1 - 2 * core
    cross = lax.rem(me + 2, 4)
    own = pl.multiple_of(core * HALF, HALF)
    oth = pl.multiple_of((1 - core) * HALF, HALF)

    def cols(c):
        return pl.ds(c * TN if isinstance(c, int) else pl.multiple_of(c * TN, TN), TN)

    def w_tile(c):
        return (
            pltpu.make_async_copy(wo.at[l, :, cols(c)], w_s.at[c, pl.ds(0, QC), :], w_sem.at[c, 0]),
            pltpu.make_async_copy(wd.at[l, :, cols(c)], w_s.at[c, pl.ds(QC, FFL), :], w_sem.at[c, 1]),
        )

    a_copy = pltpu.make_async_copy(act_hbm, act_s, a_sem.at[0])
    x_copy = pltpu.make_async_copy(x_hbm, x_s, a_sem.at[1])
    a_copy.start()
    for c in range(N_OUT):
        for d in w_tile(c):
            d.start()
    x_copy.start()

    barrier = pltpu.get_barrier_semaphore()
    pl.semaphore_signal(barrier, inc=1, device_id={"tp": sib})
    pl.semaphore_signal(barrier, inc=1, device_id={"tp": cross})
    pl.semaphore_wait(barrier, 2)

    def send_a(c):
        return pltpu.make_async_remote_copy(src_ref=part.at[c, pl.ds(oth, HALF), :], dst_ref=recv1.at[c], send_sem=s1.at[c], recv_sem=r1.at[c], device_id={"tp": sib})

    def send_b(c):
        return pltpu.make_async_remote_copy(src_ref=send2.at[c], dst_ref=recv2.at[c], send_sem=s2.at[c], recv_sem=r2.at[c], device_id={"tp": cross})

    def send_c(c):
        block = xnew.at[pl.ds(own, HALF), cols(c)]
        return pltpu.make_async_remote_copy(src_ref=block, dst_ref=block, send_sem=s3.at[c], recv_sem=r3.at[c], device_id={"tp": sib})

    def step2(c):
        send_a(c).wait_recv()
        send2[c] = (part[c, pl.ds(own, HALF), :].astype(F32) + recv1[c].astype(F32)).astype(BF16)
        send_b(c).start()

    a_copy.wait()

    @pl.loop(0, N_OUT)
    def _(c):
        for d in w_tile(c):
            d.wait()
        part[c] = jnp.dot(act_s[...], w_s[c], preferred_element_type=F32).astype(BF16)
        send_a(c).start()

        @pl.when(c >= 1)
        def _():
            step2(c - 1)

    step2(N_OUT - 1)
    x_copy.wait()

    @pl.loop(0, N_OUT)
    def _(c):
        send_b(c).wait_recv()
        total = send2[c].astype(F32) + recv2[c].astype(F32)
        xnew[pl.ds(own, HALF), cols(c)] = (x_s[pl.ds(own, HALF), cols(c)].astype(F32) + total).astype(BF16)
        send_c(c).start()

    def out_copy(c):
        return pltpu.make_async_copy(xnew.at[:, cols(c)], out_hbm.at[:, cols(c)], o_sem.at[c])

    @pl.loop(0, N_OUT)
    def _(c):
        send_c(c).wait()
        send_a(c).wait_send()
        send_b(c).wait_send()
        out_copy(c).start()

    @pl.loop(0, N_OUT)
    def _(c):
        out_copy(c).wait()


ANY = pl.BlockSpec(memory_space=pl.ANY)
VM = pl.BlockSpec(memory_space=pltpu.VMEM)
SM = pl.BlockSpec(memory_space=pltpu.SMEM)
VLIM = 62 * 1024 * 1024


def local_call(l, tables, x, kc, vc, ws, prev):
    cache = jax.ShapeDtypeStruct(kc.shape, BF16)
    n_in = 15
    return pl.pallas_call(
        functools.partial(local_kernel, l),
        name=f"layer{l}_local",
        out_shape=(jax.ShapeDtypeStruct((ROWS, ACTC), BF16), cache, cache),
        in_specs=[SM] + [VM] * 6 + [ANY] * (8 + len(prev)),
        out_specs=(ANY, ANY, ANY),
        input_output_aliases={n_in: 1, n_in + 1: 2} if prev else {},
        scratch_shapes=[
            pltpu.VMEM((ROWS, D), BF16),
            pltpu.VMEM((ROWS, D), BF16),
            pltpu.VMEM((QH, ROWS, HD), F32),
            pltpu.VMEM((KVH, ROWS, HD), F32),
            pltpu.VMEM((KVH, ROWS, HD), F32),
            pltpu.VMEM((ROWS, ACTC), BF16),
            pltpu.VMEM((NS, D, TN), BF16),
            pltpu.VMEM((NC, CB, KVH, SEQ, HD), BF16),
            pltpu.VMEM((NC, CB, KVH, SEQ, HD), BF16),
            pltpu.SemaphoreType.DMA,
            pltpu.SemaphoreType.DMA((NS, 2)),
            pltpu.SemaphoreType.DMA((NC, 2)),
            pltpu.SemaphoreType.DMA((NC, 2)),
            pltpu.SemaphoreType.DMA((N_GU + 1,)),
        ],
        compiler_params=pltpu.CompilerParams(vmem_limit_bytes=VLIM),
    )(*tables, x, kc, vc, *ws, *prev)


def reduce_call(l, act, x, wo, wd):
    sems = [pltpu.SemaphoreType.DMA((N_OUT,))] * 7
    return pl.pallas_call(
        functools.partial(reduce_kernel, l),
        name=f"layer{l}_reduce",
        out_shape=jax.ShapeDtypeStruct((ROWS, D), BF16),
        in_specs=[ANY] * 4,
        out_specs=ANY,
        scratch_shapes=[
            pltpu.VMEM((ROWS, ACTC), BF16),
            pltpu.VMEM((ROWS, D), BF16),
            pltpu.VMEM((N_OUT, ACTC, TN), BF16),
            pltpu.VMEM((N_OUT, ROWS, TN), BF16),
            pltpu.VMEM((N_OUT, HALF, TN), BF16),
            pltpu.VMEM((N_OUT, HALF, TN), BF16),
            pltpu.VMEM((N_OUT, HALF, TN), BF16),
            pltpu.VMEM((ROWS, D), BF16),
            pltpu.SemaphoreType.DMA((2,)),
            pltpu.SemaphoreType.DMA((N_OUT, 2)),
        ] + sems,
        compiler_params=pltpu.CompilerParams(vmem_limit_bytes=VLIM, collective_id=l, has_side_effects=True),
    )(act, x, wo, wd)


def solution(mesh):
    cache_spec = P(None, "dp", "tp", None, None)
    col_spec = P(None, None, "tp")
    row_spec = P(None, "tp", None)
    resid_spec = P("dp", None)
    in_specs = (resid_spec, P("dp"), cache_spec, cache_spec, P(None, None), col_spec, col_spec, col_spec, row_spec, row_spec, row_spec, col_spec, col_spec, row_spec)
    out_specs = (resid_spec, cache_spec, cache_spec)

    def local_step(residual, positions, k_cache, v_cache, ln_weight, w_q, w_k, w_v, q_norm_w, k_norm_w, w_o, w_gate, w_up, w_down):
        lane = jnp.arange(HD)
        half_ids = (lane // 2).astype(F32)
        inv_freq = ROPE_THETA ** (-2.0 * half_ids / HD)
        angles = positions.astype(F32)[:, None] * inv_freq[None, :]
        cos_b = jnp.cos(angles)
        sin_b = jnp.sin(angles) * jnp.where(lane % 2 == 0, -1.0, 1.0)[None, :]
        pos_b = jnp.broadcast_to(positions[:, None], (ROWS, HD))
        tables = (positions, ln_weight, q_norm_w, k_norm_w, cos_b, sin_b, pos_b)
        ws = (w_q, w_k, w_v, w_gate, w_up)
        x = residual
        prev = ()
        for l in range(2):
            act, *prev = local_call(l, tables, x, k_cache, v_cache, ws, tuple(prev))
            x = reduce_call(l, act, x, w_o, w_down)
        return x, prev[0], prev[1]

    return jax.shard_map(local_step, mesh=mesh, in_specs=in_specs, out_specs=out_specs, check_vma=False)
```
